32 devices in a mesh: dp: 8 (over z, x), ctx: 4 (over y, core).
Axes of the slice: x: 2, y: 2, z: 4, core: 2. Of those that a mesh axis runs over, the one named last changes fastest.
Arguments:
- queries: bfloat16 [8, 1024, 2048], P('dp', 'ctx'), may hold values from -100 to 100
- keys: bfloat16 [8, 1024, 512], P('dp', 'ctx'), may hold values from -4 to 4
- values: bfloat16 [8, 1024, 512], P('dp', 'ctx'), may hold values from -6 to 6
- segments: int32 [8, 1024], P('dp', 'ctx'), may hold values from 0 to 7, never falling along the last dimension, each value on 1 to 512 neighbouring positions
Outputs:
- attended: bfloat16 [8, 1024, 2048], P('dp', 'ctx')
The draws below stay inside these ranges and needn't reach their ends.
Inputs may be any that keep to these rules, and one draw needn't show every extreme that they name: `segments`: document numbers never fall along a packed batch, every one of the 8 documents is present, and each document has at most 512 tokens; some document has exactly 512.
All inputs are finite; a program needn't handle non-finite values.
Results may differ from the reference program's by a relative error of at most 0.0053.
Values may be sent and summed in bfloat16 or wider, within the bound.
No kernel may reach another device: no remote copies, remote signals or barrier semaphores. Data moves between devices by JAX's collectives and lax.ppermute only.
A program may use at most 192 MiB of HBM per device.

```python
import math
import jax
import jax.numpy as jnp
import numpy as np
from jax import lax

HQ = 16
HK = 4
HD = 128
SEQ_COUNT = 8
TOKENS = 1024
MOST = 512
N_DP = 8


def draw_pair(key):
    key_keys = jax.random.fold_in(key, 12)
    key_queries = jax.random.fold_in(key, 11)
    key_rows = jnp.clip(jax.random.normal(key_keys, (N_DP, TOKENS, HK * HD), jnp.float32), -4.0, 4.0)
    query_rows = jnp.clip(jax.random.normal(key_queries, (N_DP, TOKENS, HQ * HD), jnp.float32), -4.0, 4.0)
    return (query_rows, key_rows)


def draw_queries(key, part):
    return draw_pair(key)[0].astype(jnp.bfloat16)


def draw_keys(key, part):
    return draw_pair(key)[1].astype(jnp.bfloat16)


def level_of(rng, shape, cuts, smallest, largest):
    factor_of = 1.0
    for dim, blocks in cuts:
        draws = jax.random.uniform(jax.random.fold_in(jax.random.fold_in(rng, 6), dim), (blocks,), jnp.float32, smallest / len(cuts), largest / len(cuts))
        factor_of = factor_of * jnp.repeat(jnp.exp(draws), shape[dim] // blocks).reshape((-1,) + (1,) * (len(shape) - 1 - dim))
    return factor_of


def length_profile(number_of, total, bound, skew):
    loads = [(1 << 20) // math.isqrt(grade ** skew) + 1 for grade in range(2, number_of + 1)]
    spare, counts = total - bound - (number_of - 1), [1] * (number_of - 1)
    while spare > 0:
        movable = [i for i in range(number_of - 1) if counts[i] < bound]
        whole, left = sum([loads[i] for i in movable]), spare
        for i in movable:
            addition = min(bound - counts[i], max(1, left * loads[i] // whole), spare)
            counts[i] = counts[i] + addition
            spare = spare - addition
    return np.array([bound] + counts)


def ragged(own_key, number_of, total, reach, skew):
    if number_of == 2:
        one = jax.random.randint(own_key, (), max(1, total - reach), min(reach, total - 1) + 1)
        return jnp.stack([one, total - one])
    sizes = jnp.asarray(length_profile(number_of, total, reach, skew), jnp.int32)
    pairs = (number_of - 1) // 2
    giver, receiver = sizes[1:1 + 2 * pairs:2], sizes[2:2 + 2 * pairs:2]
    slack = jnp.minimum(giver - 1, reach - receiver)
    moved = jax.random.randint(jax.random.fold_in(own_key, 1), (pairs,), 0, 1 << 20) % (slack + 1)
    sizes = sizes.at[1:1 + 2 * pairs:2].set(giver - moved).at[2:2 + 2 * pairs:2].set(receiver + moved)
    return sizes[jax.random.permutation(jax.random.fold_in(own_key, 2), number_of)]


def scatter_about(stream_key, extent, scale, bound, cuts=(), held_as=jnp.bfloat16):
    entries = jax.random.normal(stream_key, extent, jnp.float32) * scale
    if len(cuts) > 0:
        entries = level_of(stream_key, extent, cuts, -0.22, 0.18) * entries
    return jnp.clip(entries, min=-bound, max=bound).astype(held_as)


def setup_inputs(seed: int = 0) -> dict:
    streams_of = jax.random.split(jax.random.key(seed), 5)
    queries = draw_queries(jax.random.fold_in(streams_of[4], 71), 0)
    keys = draw_keys(jax.random.fold_in(streams_of[4], 71), 0)
    values = scatter_about(streams_of[2], (N_DP, TOKENS, HK * HD), 1.0, 6.0, ((0, 8), (1, 4)))
    segments = jax.vmap(lambda own: jnp.searchsorted(jnp.cumsum(ragged(own, SEQ_COUNT, TOKENS, MOST, 2)), jnp.arange(TOKENS), side="right"))(jax.random.split(streams_of[3], N_DP)).reshape((N_DP, TOKENS)).astype(jnp.int32)
    return dict(queries=queries, keys=keys, values=values, segments=segments)


rope_theta = 500000.0

def rotate(values_in, positions, heads):
    rows = values_in.shape[0]
    half_dim = HD // 2
    split = values_in.astype(jnp.float32).reshape(rows, heads, HD)
    inv_freq = jnp.exp(-jnp.log(rope_theta) * 2.0 * jnp.arange(half_dim, dtype=jnp.float32) / HD)
    angles = positions.astype(jnp.float32)[:, None] * inv_freq[None, :]
    cosine_part = jnp.cos(angles)[:, None, :]
    sine_part = jnp.sin(angles)[:, None, :]
    first_half = split[..., :half_dim]
    second_half = split[..., half_dim:]
    turned = jnp.concatenate([first_half * cosine_part - second_half * sine_part, second_half * cosine_part + first_half * sine_part], axis=-1)
    return turned.reshape(rows, heads * HD).astype(jnp.bfloat16)

def doc_positions(seg_ids):
    index_all = jnp.arange(seg_ids.shape[0], dtype=jnp.int32)
    previous = jnp.concatenate([seg_ids[:1] - 1, seg_ids[:-1]])
    run_start = lax.cummax(jnp.where(seg_ids != previous, index_all, 0), axis=0)
    return index_all - run_start

def one_batch(inputs):
    query_rows, key_rows, value_rows, seg_ids = inputs
    positions = doc_positions(seg_ids)
    rot_q = rotate(query_rows, positions, HQ)
    rot_k = rotate(key_rows, positions, HK)
    block_rows = min(512, TOKENS)
    pieces = []
    for block_index in range(TOKENS // block_rows):
        q_lo = block_index * block_rows
        key_lo = max(0, q_lo - MOST)
        key_hi = q_lo + block_rows
        width = key_hi - key_lo
        query_heads = rot_q[q_lo:key_hi].astype(jnp.float32).reshape(block_rows, HK, HQ // HK, HD)
        key_heads = rot_k[key_lo:key_hi].astype(jnp.float32).reshape(width, HK, HD)
        value_heads = value_rows[key_lo:key_hi].astype(jnp.float32).reshape(width, HK, HD)
        q_index = q_lo + jnp.arange(block_rows, dtype=jnp.int32)
        k_index = key_lo + jnp.arange(width, dtype=jnp.int32)
        live_mask = (seg_ids[key_lo:key_hi][None, :] == seg_ids[q_lo:key_hi][:, None]) & (k_index[None, :] <= q_index[:, None])
        scores = jnp.einsum('thgd,shd->hgts', query_heads, key_heads) / jnp.sqrt(jnp.float32(HD))
        scores = jnp.where(live_mask, scores, jnp.float32(-1e+30))
        row_max = lax.optimization_barrier(jnp.max(scores, axis=-1, keepdims=True))
        weights = jnp.where(live_mask, jnp.exp(scores - row_max), jnp.float32(0.0))
        denom = lax.optimization_barrier(jnp.sum(weights, axis=-1))
        rounded = lax.optimization_barrier(weights.astype(jnp.bfloat16)).astype(jnp.float32)
        weighted = jnp.einsum('hgts,shd->thgd', rounded, value_heads)
        result = weighted / jnp.transpose(denom, (2, 0, 1))[..., None]
        pieces.append(result.reshape(block_rows, HQ * HD).astype(jnp.bfloat16))
    return jnp.concatenate(pieces, axis=0)

def reference(queries, keys, values, segments):
    attended = lax.map(one_batch, (queries, keys, values, segments))
    return attended
```

```python
import functools
import math

import jax
import jax.numpy as jnp
import numpy as np
from jax import lax
from jax.experimental import pallas as pl
from jax.experimental.pallas import tpu as pltpu
from jax.sharding import PartitionSpec as P

HQ = 16
HK = 4
HD = 128
GROUP = HQ // HK
ROPE_THETA = 500000.0
LANES = 128
DEAD = -1e30


def frequencies():
    half = HD // 2
    steps = np.arange(half, dtype=np.float32)
    log_theta = np.log(np.float32(ROPE_THETA))
    freq = np.exp(-log_theta * np.float32(2.0) * steps / np.float32(HD)).astype(np.float32)
    return np.concatenate([freq, freq])[None, :]


def turn_cos(turns):
    square = turns * turns
    total = jnp.full_like(square, COS_TERMS[-1])
    for term in COS_TERMS[-2::-1]:
        total = total * square + term
    return total


COS_TERMS = [
    (-1.0) ** n * (2.0 * math.pi) ** (2 * n) / math.factorial(2 * n) for n in range(11)
]
TURN = 2.0 * math.pi
TURN_HIGH = 6.28125
TURN_MID = float(np.float32(np.round((TURN - TURN_HIGH) * 2**22) / 2**22))
TURN_LOW = TURN - TURN_HIGH - TURN_MID


def cos_and_sin(positions, freq):
    angle = positions * freq
    whole = jnp.round(angle * (1.0 / TURN))
    rest = ((angle - whole * TURN_HIGH) - whole * TURN_MID) - whole * TURN_LOW
    turns = rest * (1.0 / TURN)
    lane = lax.broadcasted_iota(jnp.int32, turns.shape, 1)
    turns = jnp.where(lane < HD // 2, turns, turns - 0.25)
    turns = turns - jnp.round(turns)
    return turn_cos(turns)


def rope_factors(positions, freq):
    both = cos_and_sin(positions, freq)
    swapped = pltpu.roll(both, HD // 2, 1)
    lane = lax.broadcasted_iota(jnp.int32, both.shape, 1)
    low = lane < HD // 2
    return jnp.where(low, both, swapped), jnp.where(low, -swapped, both)


def turned(rows, cosine, sine):
    wide = rows.astype(jnp.float32)
    return (wide * cosine + pltpu.roll(wide, HD // 2, 1) * sine).astype(jnp.bfloat16)


def columns_of(row, width):
    pieces = []
    for at in range(0, width, LANES):
        size = min(LANES, width - at)
        eye = lax.broadcasted_iota(jnp.int32, (size, size), 0) == lax.broadcasted_iota(
            jnp.int32, (size, size), 1
        )
        pieces.append(
            jnp.sum(jnp.where(eye, row[:, at : at + size], 0.0), axis=1, keepdims=True)
        )
    return jnp.concatenate(pieces, axis=0)


def attend(hops, rows, mine_ref, freq_ref, *refs):
    blocks = hops + 1
    window = blocks * rows
    seg_refs = refs[:blocks]
    key_refs = refs[blocks : 2 * blocks]
    value_refs = refs[2 * blocks : 3 * blocks]
    query_ref, out_ref, cos_ref, sin_ref, bias_ref = refs[3 * blocks :]

    @pl.when(pl.program_id(0) == 0)
    def prepare():
        mine = mine_ref[0]
        parts = []
        for at in range(blocks):
            back = hops - at
            part = seg_refs[at][...].astype(jnp.float32)
            parts.append(jnp.where(mine >= back, part, -1.0))
        row = jnp.concatenate(parts, axis=1)
        column = columns_of(row, window)
        first = jnp.sum((row < column).astype(jnp.float32), axis=1, keepdims=True)
        place = lax.broadcasted_iota(jnp.int32, (window, 1), 0).astype(jnp.float32)
        cosine, sine = rope_factors(place - first, freq_ref[...])
        cos_ref[...] = cosine
        sin_ref[...] = sine
        key_place = lax.broadcasted_iota(jnp.int32, (rows, window), 1).astype(jnp.float32)
        live = (key_place >= first[hops * rows :]) & (key_place <= place[hops * rows :])
        bias_ref[...] = jnp.where(live, 0.0, DEAD)

    own = pl.ds(hops * rows, rows)
    rot_q = jnp.concatenate(
        [
            turned(query_ref[:, g * HD : (g + 1) * HD], cos_ref[own, :], sin_ref[own, :])
            for g in range(GROUP)
        ],
        axis=0,
    )
    rot_k = jnp.concatenate(
        [
            turned(
                key_refs[at][...],
                cos_ref[at * rows : (at + 1) * rows, :],
                sin_ref[at * rows : (at + 1) * rows, :],
            )
            for at in range(blocks)
        ],
        axis=0,
    )
    scores = lax.dot_general(
        rot_q, rot_k, (((1,), (1,)), ((), ())), preferred_element_type=jnp.float32
    )
    scores = scores.reshape(GROUP, rows, window) + bias_ref[...][None]
    scores = scores.reshape(GROUP * rows, window)
    top = jnp.max(scores, axis=1, keepdims=True)
    weights = jnp.exp2((scores - top) * (math.log2(math.e) / math.sqrt(HD)))
    denom = jnp.sum(weights, axis=1, keepdims=True)
    values = jnp.concatenate([ref[...] for ref in value_refs], axis=0)
    total = jnp.dot(weights.astype(jnp.bfloat16), values, preferred_element_type=jnp.float32)
    result = (total * (1.0 / denom)).astype(jnp.bfloat16)
    for g in range(GROUP):
        out_ref[:, g * HD : (g + 1) * HD] = result[g * rows : (g + 1) * rows]


def body(queries, keys, values, segments):
    rows = segments.shape[1]
    size = lax.axis_size("ctx")
    hops = size // 2
    mine = lax.axis_index("ctx").astype(jnp.int32).reshape(1)

    def behind(block, distance):
        return lax.ppermute(
            block, "ctx", [(i, i + distance) for i in range(size - distance)]
        )

    distances = list(range(hops, 0, -1))
    seg_blocks = [behind(segments, d) for d in distances] + [segments]
    key_blocks = [behind(keys[0], d) for d in distances] + [keys[0]]
    value_blocks = [behind(values[0], d) for d in distances] + [values[0]]
    blocks = hops + 1
    window = blocks * rows
    whole = pl.BlockSpec((1, rows), lambda h: (0, 0))
    head = pl.BlockSpec((rows, HD), lambda h: (0, h))
    group = pl.BlockSpec((rows, GROUP * HD), lambda h: (0, h))
    out = pl.pallas_call(
        functools.partial(attend, hops, rows),
        grid=(HK,),
        out_shape=jax.ShapeDtypeStruct((rows, HQ * HD), jnp.bfloat16),
        in_specs=[
            pl.BlockSpec(memory_space=pltpu.SMEM),
            pl.BlockSpec((1, HD), lambda h: (0, 0)),
        ]
        + [whole] * blocks
        + [head] * (2 * blocks)
        + [group],
        out_specs=group,
        scratch_shapes=[
            pltpu.VMEM((window, HD), jnp.float32),
            pltpu.VMEM((window, HD), jnp.float32),
            pltpu.VMEM((rows, window), jnp.float32),
        ],
        compiler_params=pltpu.CompilerParams(vmem_limit_bytes=48 << 20),
        name="attend",
    )(mine, jnp.asarray(frequencies()), *seg_blocks, *key_blocks, *value_blocks, queries[0])
    return out[None]


def solution(mesh):
    placed = (P("dp", "ctx", None), P("dp", "ctx", None), P("dp", "ctx", None), P("dp", "ctx"))
    return jax.shard_map(
        body, mesh=mesh, in_specs=placed, out_specs=P("dp", "ctx", None), check_vma=False
    )
```

```python
import functools
import math

import jax
import jax.numpy as jnp
import numpy as np
from jax import lax
from jax.experimental import pallas as pl
from jax.experimental.pallas import tpu as pltpu
from jax.sharding import PartitionSpec as P

HQ = 16
HK = 4
HD = 128
GROUP = HQ // HK
ROPE_THETA = 500000.0
LANES = 128
DEAD = -1e30


def frequencies():
    half = HD // 2
    steps = np.arange(half, dtype=np.float32)
    log_theta = np.log(np.float32(ROPE_THETA))
    freq = np.exp(-log_theta * np.float32(2.0) * steps / np.float32(HD)).astype(np.float32)
    return np.concatenate([freq, freq])[None, :]


TURN = 2.0 * math.pi
TURN_HIGH = 6.28125
TURN_MID = float(np.float32(np.round((TURN - TURN_HIGH) * 2**22) / 2**22))
TURN_LOW = TURN - TURN_HIGH - TURN_MID
SIN_TERMS = [(-1.0) ** n * TURN ** (2 * n + 1) / math.factorial(2 * n + 1) for n in range(7)]
SCALE = math.log2(math.e) / math.sqrt(HD)
TILE = 128


def rope_factors(positions, freq):
    angle = positions * freq
    whole = jnp.round(angle * (1.0 / TURN))
    rest = ((angle - whole * TURN_HIGH) - whole * TURN_MID) - whole * TURN_LOW
    turns = rest * (1.0 / TURN)
    lane = lax.broadcasted_iota(jnp.int32, freq.shape, 1)
    low = lane < HD // 2
    turns = turns - jnp.where(low, 0.0, 0.25)
    turns = turns - jnp.round(turns)
    part = 0.25 - jnp.abs(turns)
    square = part * part
    total = jnp.full_like(square, SIN_TERMS[-1])
    for term in SIN_TERMS[-2::-1]:
        total = total * square + term
    both = total * part
    swapped = pltpu.roll(both, HD // 2, 1)
    return jnp.where(low, both, swapped), jnp.where(low, -swapped, both)


def turned(rows, cosine, sine):
    wide = rows.astype(jnp.float32)
    return (wide * cosine + pltpu.roll(wide, HD // 2, 1) * sine).astype(jnp.bfloat16)


def column_of(row, width):
    pieces = []
    for at in range(0, width, LANES):
        size = min(LANES, width - at)
        eye = lax.broadcasted_iota(jnp.int32, (size, size), 0) == lax.broadcasted_iota(
            jnp.int32, (size, size), 1
        )
        pieces.append(
            jnp.sum(jnp.where(eye, row[:, at : at + size], 0.0), axis=1, keepdims=True)
        )
    return jnp.concatenate(pieces, axis=0)


def carried_tokens(mine, own, earlier):
    count = jnp.zeros((1, 1), jnp.float32)
    for back, row in enumerate(earlier, 1):
        same = jnp.where(row == own[:, :1], 1.0, 0.0)
        here = jnp.sum(same, axis=1, keepdims=True)
        count = count + jnp.where(mine >= back, here, 0.0)
    return count


def row_places(size):
    return lax.broadcasted_iota(jnp.int32, (size, 1), 0).astype(jnp.float32)


def lane_places(size):
    return lax.broadcasted_iota(jnp.int32, (1, size), 1).astype(jnp.float32)


def scores_of(query, keys):
    return lax.dot_general(
        query, keys, (((1,), (1,)), ((), ())), preferred_element_type=jnp.float32
    )


def group_rows(head, tile, rows):
    return [
        pl.ds((head * GROUP + g) * rows + tile * TILE, TILE) for g in range(GROUP)
    ]


def own_kernel(hops, rows, *refs):
    mine_ref, freq_hbm, own_hbm = refs[:3]
    earlier_refs = refs[3 : 3 + hops]
    query_hbm, key_hbm, value_hbm = refs[3 + hops : 6 + hops]
    rot_ref, total_ref, top_ref, denom_ref, info_ref = refs[6 + hops : 11 + hops]
    freq_ref, own_ref, query_ref, key_ref, value_ref, bias_ref, sems = refs[11 + hops :]
    first_copies = [
        pltpu.make_async_copy(own_hbm, own_ref, sems.at[3]),
        pltpu.make_async_copy(freq_hbm, freq_ref, sems.at[4]),
    ]
    copies = [
        pltpu.make_async_copy(key_hbm, key_ref, sems.at[0]),
        pltpu.make_async_copy(value_hbm, value_ref, sems.at[1]),
        pltpu.make_async_copy(query_hbm, query_ref, sems.at[2]),
    ]
    for copy in first_copies + copies:
        copy.start()
    for copy in first_copies:
        copy.wait()
    own = own_ref[...].astype(jnp.float32)
    carry = carried_tokens(
        mine_ref[0], own, [ref[...].astype(jnp.float32) for ref in earlier_refs]
    )
    inside = jnp.sum(jnp.where(own == own[:, :1], 1.0, 0.0), axis=1, keepdims=True)
    inside = jnp.where(carry > 0.0, inside, 0.0)
    info_ref[0:1, :] = freq_ref[...]
    info_ref[1:2, :] = jnp.broadcast_to(carry, (1, HD))
    info_ref[2:3, :] = jnp.broadcast_to(inside, (1, HD))
    column = column_of(own, rows)
    first = jnp.sum(jnp.where(own < column, 1.0, 0.0), axis=1, keepdims=True)
    place = row_places(rows)
    positions = place - first + jnp.where(first == 0.0, carry, 0.0)
    cosine, sine = rope_factors(positions, freq_ref[...])
    key_place = lane_places(rows)
    live = (key_place >= first) & (key_place <= place)
    bias_ref[...] = jnp.where(live, 0.0, DEAD)
    for copy in copies:
        copy.wait()

    units = [(head, tile) for head in range(HK) for tile in range(rows // TILE)]
    keys_of = {}

    def start(unit):
        head, tile = unit
        span = slice(tile * TILE, (tile + 1) * TILE)
        if head not in keys_of:
            keys_of[head] = turned(key_ref[:, head * HD : (head + 1) * HD], cosine, sine)
        parts = []
        for g, at in enumerate(group_rows(head, tile, rows)):
            lanes = slice((head * GROUP + g) * HD, (head * GROUP + g + 1) * HD)
            part = turned(query_ref[span, lanes], cosine[span], sine[span])
            rot_ref[at, :] = part
            parts.append(part)
        return scores_of(jnp.concatenate(parts, axis=0), keys_of[head][: (tile + 1) * TILE])

    def finish(unit, scores):
        head, tile = unit
        seen = (tile + 1) * TILE
        bias = bias_ref[tile * TILE : (tile + 1) * TILE, :seen]
        scores = scores.reshape(GROUP, TILE, seen) + bias[None]
        scores = scores.reshape(GROUP * TILE, seen)
        top = jnp.max(scores, axis=1, keepdims=True)
        weights = jnp.exp2((scores - top) * SCALE)
        denom = jnp.sum(weights, axis=1, keepdims=True)
        total = jnp.dot(
            weights.astype(jnp.bfloat16),
            value_ref[:seen, head * HD : (head + 1) * HD],
            preferred_element_type=jnp.float32,
        )
        top = jnp.broadcast_to(top, total.shape)
        denom = jnp.broadcast_to(denom, total.shape)
        for g, at in enumerate(group_rows(head, tile, rows)):
            piece = slice(g * TILE, (g + 1) * TILE)
            total_ref[at, :] = total[piece]
            top_ref[at, :] = top[piece]
            denom_ref[at, :] = denom[piece]

    waiting = start(units[0])
    for now, later in zip(units, units[1:] + [None]):
        following = start(later) if later is not None else None
        finish(now, waiting)
        waiting = following


def earlier_kernel(hops, rows, table, *refs):
    held = len(refs) - 11
    mine_ref, rot_ref, total_ref, top_ref, denom_ref, info_ref = refs[:6]
    block_refs = refs[6 : 6 + held]
    out_hbm, out_ref, cos_ref, sin_ref, sems = refs[6 + held :]
    mine = mine_ref[0]
    window = hops * rows
    freq = info_ref[0:1, :]
    carry = info_ref[1:2, :1]
    inside = info_ref[2:3, :1]
    cosine, sine = rope_factors(carry - window + row_places(window), freq)
    cos_ref[...] = cosine
    sin_ref[...] = sine
    key_bias = jnp.where(carry - window + lane_places(window) >= 0.0, 0.0, DEAD)

    def block(distance, lanes):
        picked = None
        for at, ref in enumerate(block_refs):
            users = [i for i in range(len(table)) if table[i].get(distance) == at]
            if not users:
                continue
            part = ref[:, lanes]
            if picked is None:
                picked = part
            else:
                wanted = functools.reduce(jnp.logical_or, [mine == i for i in users])
                picked = jnp.where(wanted, part, picked)
        return picked

    blocks_of = {}

    def start(unit):
        head, tile = unit
        if head not in blocks_of:
            keys, values = [], []
            for distance in range(hops, 0, -1):
                at = (hops - distance) * rows
                lanes = slice(head * HD, (head + 1) * HD)
                keys.append(
                    turned(
                        block(distance, lanes),
                        cos_ref[at : at + rows, :],
                        sin_ref[at : at + rows, :],
                    )
                )
                lanes = slice((HK + head) * HD, (HK + head + 1) * HD)
                values.append(block(distance, lanes))
            blocks_of[head] = (jnp.concatenate(keys, axis=0), jnp.concatenate(values, axis=0))
        query = jnp.concatenate([rot_ref[at, :] for at in group_rows(head, tile, rows)], axis=0)
        return scores_of(query, blocks_of[head][0][tile * TILE :])

    def finish(unit, scores):
        head, tile = unit
        spans = group_rows(head, tile, rows)
        live = row_places(TILE) + tile * TILE < inside
        live = jnp.concatenate([live] * GROUP, axis=0)
        scores = scores + key_bias[:, tile * TILE :]
        top = jnp.max(scores, axis=1, keepdims=True)
        old = jnp.concatenate([top_ref[at, :] for at in spans], axis=0)
        new = jnp.maximum(old, jnp.where(live, top, DEAD))
        shift = jnp.where(live, new, -DEAD)[:, :1]
        weights = jnp.exp2((scores - shift) * SCALE)
        denom = jnp.sum(weights, axis=1, keepdims=True)
        part = jnp.dot(
            weights.astype(jnp.bfloat16),
            blocks_of[head][1][tile * TILE :],
            preferred_element_type=jnp.float32,
        )
        rescale = jnp.exp2((old - new) * SCALE)
        old_denom = jnp.concatenate([denom_ref[at, :] for at in spans], axis=0)
        old_total = jnp.concatenate([total_ref[at, :] for at in spans], axis=0)
        result = (old_total * rescale + part) / (old_denom * rescale + denom)
        result = result.astype(jnp.bfloat16)
        for g in range(GROUP):
            lanes = slice((head * GROUP + g) * HD, (head * GROUP + g + 1) * HD)
            out_ref[tile * TILE : (tile + 1) * TILE, lanes] = result[
                g * TILE : (g + 1) * TILE
            ]

    units = [(head, tile) for head in range(HK) for tile in range(rows // TILE)]
    copies = []
    waiting = start(units[0])
    for now, later in zip(units, units[1:] + [None]):
        following = start(later) if later is not None else None
        finish(now, waiting)
        waiting = following
        if later is None or later[0] != now[0]:
            lanes = pl.ds(now[0] * GROUP * HD, GROUP * HD)
            copy = pltpu.make_async_copy(
                out_ref.at[:, lanes], out_hbm.at[:, lanes], sems.at[now[0]]
            )
            copy.start()
            copies.append(copy)
    for copy in copies:
        copy.wait()


def plan_rounds(size, hops):
    wanted = [(i, i + 2) for i in range(1, size - 2, 2)]
    wanted += [(i, i + 1) for i in range(0, size - 1, 2)]
    wanted += [(i, i + 2) for i in range(0, size - 2, 2)]
    for distance in range(3, hops + 1):
        wanted += [(i, i + distance) for i in range(size - distance)]
    if hops == 1:
        wanted = [(i, i + 1) for i in range(size - 1)]
    rounds, table = [], [{} for _ in range(size)]
    for source, target in wanted:
        at = 0
        while at < len(rounds) and any(s == source or t == target for s, t in rounds[at]):
            at += 1
        if at == len(rounds):
            rounds.append([])
        rounds[at].append((source, target))
        table[target][target - source] = at
    forward = []
    if hops > 1:
        for i in range(2, size, 2):
            forward.append((i + 1, i))
            table[i][1] = len(rounds)
    return rounds, forward, table


def body(queries, keys, values, segments):
    rows = segments.shape[1]
    size = lax.axis_size("ctx")
    hops = size // 2
    mine = lax.axis_index("ctx").astype(jnp.int32).reshape(1)
    rounds, forward, table = plan_rounds(size, hops)

    packed = jnp.concatenate([keys[0], values[0]], axis=1)
    with jax.named_scope("cross"):
        blocks = [lax.ppermute(packed, "ctx", pairs) for pairs in rounds]
    with jax.named_scope("numbers"):
        earlier = [
            lax.ppermute(segments, "ctx", [(i, i + d) for i in range(size - d)])
            for d in range(1, hops + 1)
        ]
    freq = jnp.asarray(frequencies())
    vmem = pl.BlockSpec(memory_space=pltpu.VMEM)
    smem = pl.BlockSpec(memory_space=pltpu.SMEM)
    hbm = pl.BlockSpec(memory_space=pltpu.HBM)
    state = jax.ShapeDtypeStruct((HQ * rows, HD), jnp.float32)
    pairs = HQ * rows * rows
    info = jax.ShapeDtypeStruct((8, HD), jnp.float32)
    rot, total, top, denom, info = pl.pallas_call(
        functools.partial(own_kernel, hops, rows),
        out_shape=[jax.ShapeDtypeStruct((HQ * rows, HD), jnp.bfloat16), state, state, state, info],
        in_specs=[smem, hbm, hbm] + [vmem] * hops + [hbm] * 3,
        out_specs=[vmem] * 5,
        scratch_shapes=[
            pltpu.VMEM((1, HD), jnp.float32),
            pltpu.VMEM((1, rows), jnp.int32),
            pltpu.VMEM((rows, HQ * HD), jnp.bfloat16),
            pltpu.VMEM((rows, HK * HD), jnp.bfloat16),
            pltpu.VMEM((rows, HK * HD), jnp.bfloat16),
            pltpu.VMEM((rows, rows), jnp.float32),
            pltpu.SemaphoreType.DMA((5,)),
        ],
        compiler_params=pltpu.CompilerParams(vmem_limit_bytes=(12 + 4 * hops) << 20),
        cost_estimate=pl.CostEstimate(
            flops=4 * HD * pairs, bytes_accessed=4 << 20, transcendentals=pairs
        ),
        name="own",
    )(mine, freq, segments, *earlier, queries[0], keys[0], values[0])
    if forward:
        ready, rot = lax.optimization_barrier((blocks[0], rot))
        with jax.named_scope("forward"):
            blocks.append(lax.ppermute(ready, "ctx", forward))
    out = pl.pallas_call(
        functools.partial(earlier_kernel, hops, rows, table),
        out_shape=jax.ShapeDtypeStruct((rows, HQ * HD), jnp.bfloat16),
        in_specs=[smem] + [vmem] * (5 + len(blocks)),
        out_specs=hbm,
        scratch_shapes=[
            pltpu.VMEM((rows, HQ * HD), jnp.bfloat16),
            pltpu.VMEM((hops * rows, HD), jnp.float32),
            pltpu.VMEM((hops * rows, HD), jnp.float32),
            pltpu.SemaphoreType.DMA((HK,)),
        ],
        compiler_params=pltpu.CompilerParams(vmem_limit_bytes=(12 + 4 * hops) << 20),
        cost_estimate=pl.CostEstimate(
            flops=4 * HD * pairs * hops,
            bytes_accessed=4 << 20,
            transcendentals=pairs * hops,
        ),
        name="earlier",
    )(mine, rot, total, top, denom, info, *blocks)
    return out[None]


def solution(mesh):
    placed = (P("dp", "ctx", None), P("dp", "ctx", None), P("dp", "ctx", None), P("dp", "ctx"))
    return jax.shard_map(
        body, mesh=mesh, in_specs=placed, out_specs=P("dp", "ctx", None), check_vma=False
    )
```

```python
import functools
import math

import jax
import jax.numpy as jnp
import numpy as np
from jax import lax
from jax.experimental import pallas as pl
from jax.experimental.pallas import tpu as pltpu
from jax.sharding import PartitionSpec as P

HQ = 16
HK = 4
HD = 128
GROUP = HQ // HK
ROPE_THETA = 500000.0
LANES = 128
DEAD = -1e30


def frequencies():
    half = HD // 2
    steps = np.arange(half, dtype=np.float32)
    log_theta = np.log(np.float32(ROPE_THETA))
    return np.exp(-log_theta * np.float32(2.0) * steps / np.float32(HD)).astype(np.float32)


def frequency_row():
    lane = lax.broadcasted_iota(jnp.int32, (1, HD), 1)
    lane = jnp.where(lane < HD // 2, lane, lane - HD // 2)
    row = jnp.zeros((1, HD), jnp.float32)
    for at, freq in enumerate(frequencies()):
        row = jnp.where(lane == at, float(freq), row)
    return row


TURN = 2.0 * math.pi
TURN_HIGH = 6.28125
TURN_MID = float(np.float32(np.round((TURN - TURN_HIGH) * 2**22) / 2**22))
TURN_LOW = TURN - TURN_HIGH - TURN_MID
SIN_TERMS = [(-1.0) ** n * TURN ** (2 * n + 1) / math.factorial(2 * n + 1) for n in range(7)]
SCALE = math.log2(math.e) / math.sqrt(HD)
TILE = 128


def rope_factors(positions, freq):
    angle = positions * freq
    whole = jnp.round(angle * (1.0 / TURN))
    rest = ((angle - whole * TURN_HIGH) - whole * TURN_MID) - whole * TURN_LOW
    turns = rest * (1.0 / TURN)
    lane = lax.broadcasted_iota(jnp.int32, freq.shape, 1)
    low = lane < HD // 2
    turns = turns - jnp.where(low, 0.0, 0.25)
    turns = turns - jnp.round(turns)
    part = 0.25 - jnp.abs(turns)
    square = part * part
    total = jnp.full_like(square, SIN_TERMS[-1])
    for term in SIN_TERMS[-2::-1]:
        total = total * square + term
    both = total * part
    swapped = pltpu.roll(both, HD // 2, 1)
    return jnp.where(low, both, swapped), jnp.where(low, -swapped, both)


def turned(rows, cosine, sine):
    wide = rows.astype(jnp.float32)
    return (wide * cosine + pltpu.roll(wide, HD // 2, 1) * sine).astype(jnp.bfloat16)


def column_of(row, width):
    pieces = []
    for at in range(0, width, LANES):
        size = min(LANES, width - at)
        eye = lax.broadcasted_iota(jnp.int32, (size, size), 0) == lax.broadcasted_iota(
            jnp.int32, (size, size), 1
        )
        pieces.append(
            jnp.sum(jnp.where(eye, row[:, at : at + size], 0.0), axis=1, keepdims=True)
        )
    return jnp.concatenate(pieces, axis=0)


def carried_tokens(mine, own, earlier):
    count = jnp.zeros((1, 1), jnp.float32)
    for back, row in enumerate(earlier, 1):
        same = jnp.where(row == own[:, :1], 1.0, 0.0)
        here = jnp.sum(same, axis=1, keepdims=True)
        count = count + jnp.where(mine >= back, here, 0.0)
    return count


def row_places(size):
    return lax.broadcasted_iota(jnp.int32, (size, 1), 0).astype(jnp.float32)


def lane_places(size):
    return lax.broadcasted_iota(jnp.int32, (1, size), 1).astype(jnp.float32)


def scores_of(keys, query):
    return lax.dot_general(
        keys, query, (((1,), (1,)), ((), ())), preferred_element_type=jnp.float32
    )


def flipped(block):
    return jnp.transpose(block)


def pipelined(units, start, finish):
    waiting = start(units[0])
    for now, later in zip(units, units[1:] + [None]):
        following = start(later) if later is not None else None
        finish(now, waiting)
        waiting = following


def own_kernel(hops, rows, *refs):
    mine_ref, own_ref = refs[:2]
    earlier_refs = refs[2 : 2 + hops]
    query_ref, block_ref = refs[2 + hops : 4 + hops]
    rot_ref, total_ref, top_ref, denom_ref, info_ref, bias_ref = refs[4 + hops :]
    own = own_ref[...].astype(jnp.float32)
    carry = carried_tokens(
        mine_ref[0], own, [ref[...].astype(jnp.float32) for ref in earlier_refs]
    )
    inside = jnp.sum(jnp.where(own == own[:, :1], 1.0, 0.0), axis=1, keepdims=True)
    inside = jnp.where(carry > 0.0, inside, 0.0)
    info_ref[0:1, :] = jnp.broadcast_to(carry, (1, HD))
    info_ref[1:2, :] = jnp.broadcast_to(inside, (1, HD))
    column = column_of(own, rows)
    first = jnp.sum(jnp.where(own < column, 1.0, 0.0), axis=1, keepdims=True)
    place = row_places(rows)
    positions = place - first + jnp.where(first == 0.0, carry, 0.0)
    cosine, sine = rope_factors(positions, frequency_row())
    first_row = jnp.sum(jnp.where(column < own, 1.0, 0.0), axis=0, keepdims=True)
    live = (place >= first_row) & (place <= lane_places(rows))
    bias_ref[...] = jnp.where(live, 0.0, DEAD)
    held = {}

    def start(unit):
        head = unit // GROUP
        if head not in held:
            lanes = slice(head * HD, (head + 1) * HD)
            keys = turned(block_ref[:, lanes], cosine, sine)
            lanes = slice((HK + head) * HD, (HK + head + 1) * HD)
            held[head] = (keys, flipped(block_ref[:, lanes]))
        at = slice(unit * rows, (unit + 1) * rows)
        query = turned(query_ref[:, unit * HD : (unit + 1) * HD], cosine, sine)
        rot_ref[at, :] = query
        return scores_of(held[head][0], query)

    def finish(unit, scores):
        pieces, tops, denoms = [], [], []
        for tile in range(rows // TILE):
            seen = (tile + 1) * TILE
            lanes = slice(tile * TILE, seen)
            part = scores[:seen, lanes] + bias_ref[:seen, lanes]
            top = jnp.max(part, axis=0, keepdims=True)
            weights = jnp.exp2((part - top) * SCALE)
            denoms.append(jnp.sum(weights, axis=0, keepdims=True))
            tops.append(top)
            weights = weights.astype(jnp.bfloat16)
            if seen < rows:
                rest = jnp.zeros((rows - seen, TILE), jnp.bfloat16)
                weights = jnp.concatenate([weights, rest], axis=0)
            pieces.append(weights)
        weights = jnp.concatenate(pieces, axis=1)
        total = jnp.dot(held[unit // GROUP][1], weights, preferred_element_type=jnp.float32)
        total_ref[unit * HD : (unit + 1) * HD, :] = total
        top_ref[unit : unit + 1, :] = jnp.concatenate(tops, axis=1)
        denom_ref[unit : unit + 1, :] = jnp.concatenate(denoms, axis=1)

    pipelined(list(range(HQ)), start, finish)


def earlier_kernel(hops, rows, table, *refs):
    held = len(refs) - 13
    mine_ref, rot_ref, total_ref, top_ref, denom_ref, info_ref = refs[:6]
    block_refs = refs[6 : 6 + held]
    out_hbm, out_ref, cos_ref, sin_ref, key_side_ref, query_side_ref, sems = refs[6 + held :]
    mine = mine_ref[0]
    window = hops * rows
    carry = info_ref[0:1, :1]
    inside = info_ref[1:2, :1]
    key_positions = carry - window + row_places(window)
    cosine, sine = rope_factors(key_positions, frequency_row())
    cos_ref[...] = cosine
    sin_ref[...] = sine
    lane = lane_places(HD)
    key_bias = jnp.where(key_positions >= 0.0, 0.0, DEAD)
    key_side = jnp.where(lane == 0.0, key_bias, jnp.where(lane == 1.0, 1.0, 0.0))
    key_side_ref[...] = key_side.astype(jnp.bfloat16)
    query_bias = jnp.where(row_places(rows) < inside, 0.0, DEAD)
    query_side = jnp.where(lane == 0.0, 1.0, jnp.where(lane == 1.0, query_bias, 0.0))
    query_side_ref[...] = query_side.astype(jnp.bfloat16)

    def block(distance, lanes):
        picked = None
        for at, ref in enumerate(block_refs):
            users = [i for i in range(len(table)) if table[i].get(distance) == at]
            if not users:
                continue
            part = ref[:, lanes]
            if picked is None:
                picked = part
            else:
                wanted = functools.reduce(jnp.logical_or, [mine == i for i in users])
                picked = jnp.where(wanted, part, picked)
        return picked

    blocks_of = {}
    copies = []

    def start(unit):
        head = unit // GROUP
        if head not in blocks_of:
            keys, values = [], []
            for distance in range(hops, 0, -1):
                at = (hops - distance) * rows
                lanes = slice(head * HD, (head + 1) * HD)
                keys.append(
                    turned(
                        block(distance, lanes),
                        cos_ref[at : at + rows, :],
                        sin_ref[at : at + rows, :],
                    )
                )
                lanes = slice((HK + head) * HD, (HK + head + 1) * HD)
                values.append(flipped(block(distance, lanes)))
            keys = jnp.concatenate([jnp.concatenate(keys, axis=0), key_side_ref[...]], axis=1)
            blocks_of[head] = (keys, jnp.concatenate(values, axis=1))
        query = rot_ref[unit * rows : (unit + 1) * rows, :]
        query = jnp.concatenate([query, query_side_ref[...]], axis=1)
        return scores_of(blocks_of[head][0], query)

    def finish(unit, scores):
        head = unit // GROUP
        pieces, rescales, denoms = [], [], []
        for tile in range(rows // TILE):
            skip = tile * TILE
            lanes = slice(skip, skip + TILE)
            part = scores[skip:, lanes]
            top = jnp.max(part, axis=0, keepdims=True)
            old = top_ref[unit : unit + 1, lanes]
            new = jnp.maximum(old, top)
            weights = jnp.exp2((part - new) * SCALE)
            rescale = jnp.exp2((old - new) * SCALE)
            denoms.append(
                denom_ref[unit : unit + 1, lanes] * rescale
                + jnp.sum(weights, axis=0, keepdims=True)
            )
            rescales.append(rescale)
            weights = weights.astype(jnp.bfloat16)
            if skip > 0:
                rest = jnp.zeros((skip, TILE), jnp.bfloat16)
                weights = jnp.concatenate([rest, weights], axis=0)
            pieces.append(weights)
        weights = jnp.concatenate(pieces, axis=1)
        part = jnp.dot(blocks_of[head][1], weights, preferred_element_type=jnp.float32)
        rescale = jnp.concatenate(rescales, axis=1)
        inverse = 1.0 / jnp.concatenate(denoms, axis=1)
        result = (total_ref[unit * HD : (unit + 1) * HD, :] * rescale + part) * inverse
        out_ref[:, unit * HD : (unit + 1) * HD] = jnp.transpose(result).astype(jnp.bfloat16)
        if unit % GROUP == GROUP - 1:
            lanes = pl.ds(head * GROUP * HD, GROUP * HD)
            copy = pltpu.make_async_copy(
                out_ref.at[:, lanes], out_hbm.at[:, lanes], sems.at[head]
            )
            copy.start()
            copies.append(copy)

    pipelined(list(range(HQ)), start, finish)
    for copy in copies:
        copy.wait()


def plan_rounds(size, hops):
    wanted = [(i, i + 2) for i in range(1, size - 2, 2)]
    wanted += [(i, i + 1) for i in range(0, size - 1, 2)]
    wanted += [(i, i + 2) for i in range(0, size - 2, 2)]
    for distance in range(3, hops + 1):
        wanted += [(i, i + distance) for i in range(size - distance)]
    if hops == 1:
        wanted = [(i, i + 1) for i in range(size - 1)]
    rounds, table = [], [{} for _ in range(size)]
    for source, target in wanted:
        at = 0
        while at < len(rounds) and any(s == source or t == target for s, t in rounds[at]):
            at += 1
        if at == len(rounds):
            rounds.append([])
        rounds[at].append((source, target))
        table[target][target - source] = at
    forward = []
    if hops > 1:
        for i in range(2, size, 2):
            forward.append((i + 1, i))
            table[i][1] = len(rounds)
    return rounds, forward, table


def body(queries, keys, values, segments):
    rows = segments.shape[1]
    size = lax.axis_size("ctx")
    hops = size // 2
    mine = lax.axis_index("ctx").astype(jnp.int32).reshape(1)
    rounds, forward, table = plan_rounds(size, hops)

    packed = jnp.concatenate([keys[0], values[0]], axis=1)
    with jax.named_scope("cross"):
        blocks = [lax.ppermute(packed, "ctx", pairs) for pairs in rounds]
    with jax.named_scope("numbers"):
        earlier = [
            lax.ppermute(segments, "ctx", [(i, i + d) for i in range(size - d)])
            for d in range(1, hops + 1)
        ]
    forwarded = blocks[0]
    if forward:
        forwarded, *earlier = lax.optimization_barrier((forwarded, *earlier))
        with jax.named_scope("forward"):
            blocks.append(lax.ppermute(forwarded, "ctx", forward))
    vmem = pl.BlockSpec(memory_space=pltpu.VMEM)
    smem = pl.BlockSpec(memory_space=pltpu.SMEM)
    hbm = pl.BlockSpec(memory_space=pltpu.HBM)
    wide_queries = queries[0].astype(jnp.float32)
    per_head = jax.ShapeDtypeStruct((HQ, rows), jnp.float32)
    pairs = HQ * rows * rows
    rot, total, top, denom, info = pl.pallas_call(
        functools.partial(own_kernel, hops, rows),
        out_shape=[
            jax.ShapeDtypeStruct((HQ * rows, HD), jnp.bfloat16),
            jax.ShapeDtypeStruct((HQ * HD, rows), jnp.float32),
            per_head,
            per_head,
            jax.ShapeDtypeStruct((8, HD), jnp.float32),
        ],
        in_specs=[smem] + [vmem] * (3 + hops),
        out_specs=[vmem] * 5,
        scratch_shapes=[pltpu.VMEM((rows, rows), jnp.float32)],
        compiler_params=pltpu.CompilerParams(vmem_limit_bytes=16 << 20),
        cost_estimate=pl.CostEstimate(
            flops=4 * HD * pairs, bytes_accessed=4 << 20, transcendentals=pairs
        ),
        name="own",
    )(mine, segments.astype(jnp.float32), *earlier, wide_queries, packed)
    out = pl.pallas_call(
        functools.partial(earlier_kernel, hops, rows, table),
        out_shape=jax.ShapeDtypeStruct((rows, HQ * HD), jnp.bfloat16),
        in_specs=[smem] + [vmem] * (5 + len(blocks)),
        out_specs=hbm,
        scratch_shapes=[
            pltpu.VMEM((rows, HQ * HD), jnp.bfloat16),
            pltpu.VMEM((hops * rows, HD), jnp.float32),
            pltpu.VMEM((hops * rows, HD), jnp.float32),
            pltpu.VMEM((hops * rows, HD), jnp.bfloat16),
            pltpu.VMEM((rows, HD), jnp.bfloat16),
            pltpu.SemaphoreType.DMA((HK,)),
        ],
        compiler_params=pltpu.CompilerParams(vmem_limit_bytes=(8 + 4 * hops) << 20),
        cost_estimate=pl.CostEstimate(
            flops=4 * HD * pairs * hops,
            bytes_accessed=4 << 20,
            transcendentals=pairs * hops,
        ),
        name="earlier",
    )(mine, rot, total, top, denom, info, *blocks)
    return out[None]


def solution(mesh):
    placed = (P("dp", "ctx", None), P("dp", "ctx", None), P("dp", "ctx", None), P("dp", "ctx"))
    return jax.shard_map(
        body, mesh=mesh, in_specs=placed, out_specs=P("dp", "ctx", None), check_vma=False
    )
```
